32 devices in a mesh: high: 8 (over z, core), low: 4 (over y, x).
Axes of the slice: x: 2, y: 2, z: 4, core: 2. Of those that a mesh axis runs over, the one named last changes fastest.
Arguments:
- wave_parts: float32 [2, 128, 128, 128], P(None, ('high', 'low')), may hold values from -6 to 6
- level_table: float32 [128, 128, 128], P(('high', 'low')), may hold values from -2 to 2
- phase_angles: float32 [2, 128], replicated, may hold values from 0.3 to 1.2
- mix_angles: float32 [2, 4], replicated, may hold values from 0.3 to 1.2
Outputs:
- result_parts: float32 [2, 128, 128, 128], P(None, ('high', 'low'))
- marginal: float32 [16, 128, 128], P('low', 'high')
The draws below stay inside these ranges and needn't reach their ends.
All inputs are finite; a program needn't handle non-finite values.
Results may differ from the reference program's by a relative error of at most 0.0003.
Values sent between devices are 32-bit elements; how exact they have to be, the bound alone decides.
A program may use at most 64 MiB of HBM per device.

```python
import jax
import jax.numpy as jnp
from jax import lax

BLOCKS_DEV = 4
ROWS = 128
LANES = 128
BLOCKS = 128
LAYERS = 2
N_HIGH = 8
N_LOW = 4


def block_scale(stream_key, extent, cuts, least, high):
    factor_of = 1.0
    for dim, blocks in cuts:
        heights = jax.random.uniform(jax.random.fold_in(jax.random.fold_in(stream_key, 6), dim), (blocks,), jnp.float32, least / len(cuts), high / len(cuts))
        factor_of = factor_of * jnp.repeat(jnp.exp(heights), extent[dim] // blocks).reshape((-1,) + (1,) * (len(extent) - 1 - dim))
    return factor_of


def normal_values(key, extent, deviation, most, split=(), kind=jnp.bfloat16):
    level = block_scale(key, extent, split, -0.22, 0.18) if split else 1.0
    values = jax.random.normal(key, extent, jnp.float32) * deviation * level
    return jnp.minimum(jnp.maximum(values, -most), most).astype(kind)


def setup_inputs(seed: int = 0) -> dict:
    streams_of = jax.random.split(jax.random.key(seed), 5)
    wave_parts = normal_values(streams_of[0], (2, BLOCKS, ROWS, LANES), 1.0, 6.0, ((1, 32),), jnp.float32)
    level_table = jnp.clip(jax.random.uniform(streams_of[1], (BLOCKS, ROWS, LANES), jnp.float32, -2.0, 2.0) * block_scale(streams_of[1], (BLOCKS, ROWS, LANES), ((0, 32),), -0.4, 0.0), -2.0, 2.0)
    phase_angles = jnp.clip(jax.random.uniform(streams_of[2], (LAYERS, LANES), jnp.float32, 0.3, 1.2), 0.3, 1.2)
    mix_angles = jnp.clip(jax.random.uniform(streams_of[3], (LAYERS, 4), jnp.float32, 0.3, 1.2), 0.3, 1.2)
    return dict(wave_parts=wave_parts, level_table=level_table, phase_angles=phase_angles, mix_angles=mix_angles)


def count_bits(values, count):
    places = jnp.arange(count.bit_length() - 1, dtype=jnp.int32)
    return jnp.sum((values[..., None] >> places) & 1, axis=-1)


def real_turn_table(count, angle):
    rank = jnp.arange(count, dtype=jnp.int32)
    apart = count_bits(rank[:, None] ^ rank[None, :], count)
    minus = count_bits(rank[:, None] & (rank[:, None] ^ rank[None, :]), count)
    bits = count.bit_length() - 1
    size = jnp.cos(angle) ** (bits - apart).astype(jnp.float32) * jnp.sin(angle) ** apart.astype(jnp.float32)
    return size * jnp.where(minus % 2 == 1, -1.0, 1.0).astype(jnp.float32)


def apply_along(values, dim, angle):
    real_part = real_turn_table(values.shape[dim], angle)
    def times(table):
        moved = jnp.tensordot(values, table, axes=([dim], [0]), precision=lax.Precision.HIGHEST)
        return jnp.moveaxis(moved, -1, dim)
    return times(real_part)


def phase_step(values, levels, angle):
    turn = angle * levels
    return jnp.stack([values[0] * jnp.cos(turn) + values[1] * jnp.sin(turn), values[1] * jnp.cos(turn) - values[0] * jnp.sin(turn)])


def reference(wave_parts, level_table, phase_angles, mix_angles):
    values = wave_parts
    for layer in range(LAYERS):
        values = phase_step(values, level_table, phase_angles[layer])
        values = apply_along(values, 3, mix_angles[layer, 0])
        values = apply_along(values, 2, mix_angles[layer, 1])
        parts = values.reshape(2, N_HIGH, N_LOW, BLOCKS_DEV, ROWS, LANES)
        parts = apply_along(parts, 1, mix_angles[layer, 2])
        parts = apply_along(parts, 2, mix_angles[layer, 3])
        parts = apply_along(parts, 3, mix_angles[layer, 2])
        values = parts.reshape(values.shape)
    chance = values[0] * values[0] + values[1] * values[1]
    marginal = jnp.mean(chance.reshape(N_HIGH, -1, ROWS, LANES), axis=0)
    return values, marginal
```

```python
import functools

import jax
import jax.numpy as jnp
from jax import lax
from jax.experimental import pallas as pl
from jax.experimental.pallas import tpu as pltpu
from jax.sharding import PartitionSpec as P

LAYERS = 2
MESH = pl.DeviceIdType.MESH
SUBLANES = 8
TERMS = 5


def count_bits(values, count):
    places = jnp.arange(count.bit_length() - 1, dtype=jnp.int32)
    return jnp.sum(values[..., None] >> places & 1, axis=-1)


def real_turn_table(count, angle):
    rank = jnp.arange(count, dtype=jnp.int32)
    apart = count_bits(rank[:, None] ^ rank[None, :], count)
    minus = count_bits(rank[:, None] & (rank[:, None] ^ rank[None, :]), count)
    bits = count.bit_length() - 1
    size = jnp.cos(angle) ** (bits - apart).astype(jnp.float32) * jnp.sin(angle) ** apart.astype(
        jnp.float32
    )
    return size * jnp.where(minus % 2 == 1, -1.0, 1.0).astype(jnp.float32)


def apply_along(values, dim, angle):
    real_part = real_turn_table(values.shape[dim], angle)
    moved = jnp.tensordot(values, real_part, axes=([dim], [0]), precision=lax.Precision.HIGHEST)
    return jnp.moveaxis(moved, -1, dim)


def phase_step(values, levels, angle):
    turn = angle * levels
    return jnp.stack(
        [
            values[0] * jnp.cos(turn) + values[1] * jnp.sin(turn),
            values[1] * jnp.cos(turn) - values[0] * jnp.sin(turn),
        ]
    )


def by_axis(wave_parts, level_table, phase_angles, mix_angles):
    values = wave_parts
    for layer in range(LAYERS):
        values = phase_step(values, level_table, phase_angles[layer])
        values = apply_along(values, 3, mix_angles[layer, 0])
        values = apply_along(values, 2, mix_angles[layer, 1])
        values = apply_along(values, 1, mix_angles[layer, 2])
        moved = lax.all_to_all(values, "high", split_axis=2, concat_axis=1, tiled=True)
        spread = moved.reshape(2, lax.axis_size("high"), -1, moved.shape[2], moved.shape[3])
        moved = apply_along(spread, 1, mix_angles[layer, 2]).reshape(moved.shape)
        values = lax.all_to_all(moved, "high", split_axis=1, concat_axis=2, tiled=True)
        moved = lax.all_to_all(values, "low", split_axis=3, concat_axis=1, tiled=True)
        spread = moved.reshape(2, lax.axis_size("low"), -1, moved.shape[2], moved.shape[3])
        moved = apply_along(spread, 1, mix_angles[layer, 3]).reshape(moved.shape)
        values = lax.all_to_all(moved, "low", split_axis=1, concat_axis=3, tiled=True)
    chance = values[0] * values[0] + values[1] * values[1]
    marginal = lax.psum_scatter(chance, "high", scatter_dimension=1, tiled=True) / lax.axis_size(
        "high"
    )
    return (values, marginal)


def mix_list(values, groups):
    values = list(values)
    stride = 1
    for bits, cos, sin in groups:
        for _ in range(bits):
            for at in range(len(values)):
                if at & stride == 0:
                    u, v = values[at], values[at + stride]
                    values[at] = cos * u - sin * v
                    values[at + stride] = cos * v + sin * u
            stride *= 2
    return values


def series(square, first):
    terms = [1.0]
    for n in range(TERMS):
        terms.append(-terms[-1] / ((2 * n + first) * (2 * n + first + 1)))
    out = jnp.full_like(square, terms[-1])
    for term in terms[-2::-1]:
        out = out * square + term
    return out


def cos_sin(half):
    square = half * half
    cos, sin = series(square, 1), half * series(square, 2)
    twice = sin + sin
    return 1.0 - twice * sin, twice * cos


def turn_matrix(groups, sign):
    size = 1
    for bits, _, _ in groups:
        size <<= bits
    row = lax.broadcasted_iota(jnp.int32, (size, size), 0)
    column = lax.broadcasted_iota(jnp.int32, (size, size), 1)
    out = None
    place = 0
    for bits, cos, sin in groups:
        up = sign * sin
        for _ in range(bits):
            kb = (row >> place) & 1
            nb = (column >> place) & 1
            factor = jnp.where(kb == nb, cos, jnp.where(nb > kb, up, -up))
            out = factor if out is None else out * factor
            place += 1
    return out


def split(values):
    high = values.astype(jnp.bfloat16)
    return high, (values - high.astype(jnp.float32)).astype(jnp.bfloat16)


def dot(left, right):
    return jnp.dot(left, right, preferred_element_type=jnp.float32)


def log2(count):
    return count.bit_length() - 1


def turn_chunks(ref, t, h, part, pair):
    chunks = part // SUBLANES
    at = [pl.ds(h * part + j * SUBLANES, SUBLANES) for j in range(chunks)]
    return [mix_list([ref[p, t, r, :] for r in at], [(log2(chunks), *pair)]) for p in range(2)]


def finish(back, total, out_hbm, marginal_hbm, sem):
    copies = [
        pltpu.make_async_copy(back, out_hbm, sem.at[0]),
        pltpu.make_async_copy(total, marginal_hbm, sem.at[1]),
    ]
    for copy in copies:
        copy.start()
    for copy in copies:
        copy.wait()


def kernel(
    n_high, n_low,
    mix_ref, wave_hbm, level_hbm, phase_ref,
    back, total,
    wave_ref, level_ref, a_ref, b_ref, c_ref, level_b, chance, pair, sums, gathered,
    load_sem, send_sem, recv_state, recv_level, recv_back, recv_pair, recv_sums,
):
    loads = [
        pltpu.make_async_copy(level_hbm, level_ref, load_sem.at[0]),
        pltpu.make_async_copy(wave_hbm, wave_ref, load_sem.at[1]),
    ]
    for load in loads:
        load.start()
    _, blocks, rows, lanes = wave_ref.shape
    part = rows // n_high
    chunks = part // SUBLANES
    count = n_high * n_low
    twos = n_high // 2
    mh, ml = lax.axis_index("high"), lax.axis_index("low")

    barrier = pltpu.get_barrier_semaphore()

    def other(i):
        k = 1 + i
        return k, (mh + k // n_low) % n_high, (ml + k % n_low) % n_low

    @pl.loop(0, count - 1)
    def _(i):
        _, dh, dl = other(i)
        pl.semaphore_signal(barrier, inc=1, device_id=(dh, dl), device_id_type=MESH)

    def angles(layer, group):
        angle = jnp.full((SUBLANES, lanes), mix_ref[layer, group], jnp.float32)
        return jnp.cos(angle), jnp.sin(angle)

    def wide(pair, size):
        return tuple(jnp.broadcast_to(x[:1, :1], (size, size)) for x in pair)

    def phase(re, im, levels, layer):
        cos, sin = cos_sin(phase_ref[pl.ds(layer, 1), :] * 0.5 * levels)
        return re * cos + im * sin, im * cos - re * sin

    def tile(h, j):
        return pl.ds(pl.multiple_of(h * part + j * SUBLANES, SUBLANES), SUBLANES)

    def mix_in_a(ref, j, layer):
        row_pair, block_pair = angles(layer, 1), angles(layer, 2)
        groups = [(log2(n_high), *row_pair), (log2(blocks), *block_pair)]
        at = [(t, tile(h, j)) for t in range(blocks) for h in range(n_high)]
        for p in range(2):
            values = mix_list([ref[p, t, r, :] for t, r in at], groups)
            for (t, r), value in zip(at, values):
                ref[p, t, r, :] = value

    def mix_chunks(ref, t, h, layer):
        return turn_chunks(ref, t, h, part, angles(layer, 1))

    def tables(layer):
        lane = split(turn_matrix([(log2(lanes), *wide(angles(layer, 0), lanes))], 1.0))
        packed = jnp.concatenate(
            [jnp.concatenate(lane, axis=1), jnp.concatenate([lane[0], jnp.zeros_like(lane[0])], axis=1)], axis=0
        )
        size = count * SUBLANES
        row_pair, block_pair, low_pair = (wide(angles(layer, g), size) for g in (1, 2, 3))
        upper = turn_matrix(
            [(log2(SUBLANES), *row_pair), (log2(n_high), *block_pair), (log2(n_low), *low_pair)], -1.0
        )
        return packed, split(upper)

    def mix_in_b(ref, j, packed, upper):
        size = count * SUBLANES
        both = jnp.concatenate([ref[j, p].reshape(size, lanes) for p in range(2)], axis=1)
        high, low = split(both)
        both = dot(upper[0], high) + (dot(upper[1], high) + dot(upper[0], low))
        rows = jnp.concatenate([both[:, :lanes], both[:, lanes:]], axis=0)
        out = dot(jnp.concatenate(split(rows), axis=1), packed)
        out = out[:, :lanes] + out[:, lanes:]
        for p in range(2):
            c_ref[j, p] = out[p * size : (p + 1) * size].reshape(n_low, n_high, SUBLANES, lanes)

    for load in loads:
        load.wait()

    @pl.loop(0, blocks * rows // 32)
    def _(i):
        t, r = i // (rows // 32), pl.ds(pl.multiple_of(i % (rows // 32) * 32, 32), 32)
        re, im = phase(wave_ref[0, t, r, :], wave_ref[1, t, r, :], level_ref[t, r, :], 0)
        a_ref[0, t, r, :] = re
        a_ref[1, t, r, :] = im

    pl.semaphore_wait(barrier, count - 1)

    def state_copy(j, i):
        k, dh, dl = other(i)
        return pltpu.make_async_remote_copy(
            src_ref=a_ref.at[:, dl, tile(dh, j), :],
            dst_ref=b_ref.at[j, :, ml, mh],
            send_sem=send_sem.at[0],
            recv_sem=recv_state.at[j, k],
            device_id=(dh, dl),
            device_id_type=MESH,
        )

    def level_copy(j, i):
        k, dh, dl = other(i)
        return pltpu.make_async_remote_copy(
            src_ref=level_ref.at[dl, tile(dh, j), :],
            dst_ref=level_b.at[j, ml, mh],
            send_sem=send_sem.at[1],
            recv_sem=recv_level.at[j, k],
            device_id=(dh, dl),
            device_id_type=MESH,
        )

    def back_copy(j, i):
        k, dh, dl = other(i)
        return pltpu.make_async_remote_copy(
            src_ref=c_ref.at[j, :, dl, dh],
            dst_ref=back.at[:, ml, tile(mh, j), :],
            send_sem=send_sem.at[2],
            recv_sem=recv_back.at[j, k],
            device_id=(dh, dl),
            device_id_type=MESH,
        )

    def each(do, copy, j):
        @pl.loop(0, count - 1)
        def _(i):
            getattr(copy(j, i), do)()

    each("start", level_copy, 0)

    @pl.loop(0, chunks)
    def _(j):
        mix_in_a(a_ref, j, 0)

    @pl.loop(0, blocks)
    def _(t):
        for h in range(n_high):
            for p, values in enumerate(mix_chunks(a_ref, t, h, 0)):
                for j, value in enumerate(values):
                    a_ref[p, t, tile(h, j), :] = value

    for j in range(chunks):
        each("start", state_copy, j)
        if j:
            each("start", level_copy, j)
    first, second = tables(0), tables(1)
    for j in range(chunks):
        b_ref[j, :, ml, mh] = a_ref[:, ml, tile(mh, j), :]
        level_b[j, ml, mh] = level_ref[ml, tile(mh, j), :]

    for j in range(chunks):
        each("wait_recv", state_copy, j)
        mix_in_b(b_ref, j, *first)
        each("wait_recv", level_copy, j)

        @pl.loop(0, n_low)
        def _(l):
            re, im = phase(c_ref[j, 0, l], c_ref[j, 1, l], level_b[j, l], 1)
            c_ref[j, 0, l] = re
            c_ref[j, 1, l] = im

        mix_in_b(c_ref, j, *second)
        each("start", back_copy, j)
        back[:, ml, tile(mh, j), :] = c_ref[j, :, ml, mh]

    for j in range(chunks):
        each("wait_recv", back_copy, j)
        mix_in_a(back, j, 1)

    @pl.loop(0, blocks)
    def _(t):
        for h in range(n_high):
            re, im = mix_chunks(back, t, h, 1)
            for j in range(chunks):
                back[0, t, tile(h, j), :] = re[j]
                back[1, t, tile(h, j), :] = im[j]
                chance[h % 2, h // 2, t, pl.ds(j * SUBLANES, SUBLANES), :] = re[j] * re[j] + im[j] * im[j]

    mz, mc = mh // 2, mh % 2

    def pair_copy(i):
        dz = (mz + i + 1) % twos
        return dz, pltpu.make_async_remote_copy(
            src_ref=chance.at[1 - mc, dz],
            dst_ref=pair.at[dz],
            send_sem=send_sem.at[3],
            recv_sem=recv_pair.at[i],
            device_id=(mz * 2 + 1 - mc, ml),
            device_id_type=MESH,
        )

    def sums_copy(i):
        dz = (mz + i + 1) % twos
        return pltpu.make_async_remote_copy(
            src_ref=sums.at[dz],
            dst_ref=gathered.at[mz],
            send_sem=send_sem.at[4],
            recv_sem=recv_sums.at[i],
            device_id=(dz * 2 + mc, ml),
            device_id_type=MESH,
        )

    for i in range(twos):
        pair_copy(i)[1].start()
    for i in range(twos):
        dz, copy = pair_copy(i)
        copy.wait_recv()
        summed = chance[mc, dz] + pair[dz]
        if i < twos - 1:
            sums[dz] = summed
            sums_copy(i).start()
        else:
            gathered[dz] = summed
    for i in range(twos - 1):
        sums_copy(i).wait_recv()
    summed = gathered[0]
    for z in range(1, twos):
        summed = summed + gathered[z]
    total[...] = summed * (1.0 / n_high)
    for j in range(chunks):
        each("wait_send", state_copy, j)
        each("wait_send", level_copy, j)
        each("wait_send", back_copy, j)
    for i in range(twos):
        pair_copy(i)[1].wait_send()
    for i in range(twos - 1):
        sums_copy(i).wait_send()


def on_device(n_high, n_low, wave_parts, level_table, phase_angles, mix_angles):
    _, blocks, rows, lanes = wave_parts.shape
    if blocks != n_low or n_high % 2 or rows % (n_high * SUBLANES):
        return by_axis(wave_parts, level_table, phase_angles, mix_angles)
    part = rows // n_high
    chunks = part // SUBLANES
    count = n_high * n_low
    f32 = jnp.float32
    vmem = pl.BlockSpec(memory_space=pltpu.VMEM)
    any_space = pl.BlockSpec(memory_space=pl.ANY)
    smem = pl.BlockSpec(memory_space=pltpu.SMEM)
    back, total = pl.pallas_call(
        functools.partial(kernel, n_high, n_low),
        out_shape=[
            pltpu.VMEM(wave_parts.shape, f32),
            pltpu.VMEM((blocks, part, lanes), f32),
        ],
        in_specs=[smem, any_space, any_space, vmem],
        out_specs=[vmem, vmem],
        scratch_shapes=[
            pltpu.VMEM((2, blocks, rows, lanes), f32),
            pltpu.VMEM((blocks, rows, lanes), f32),
            pltpu.VMEM((2, blocks, rows, lanes), f32),
            pltpu.VMEM((chunks, 2, n_low, n_high, SUBLANES, lanes), f32),
            pltpu.VMEM((chunks, 2, n_low, n_high, SUBLANES, lanes), f32),
            pltpu.VMEM((chunks, n_low, n_high, SUBLANES, lanes), f32),
            pltpu.VMEM((2, n_high // 2, blocks, part, lanes), f32),
            pltpu.VMEM((n_high // 2, blocks, part, lanes), f32),
            pltpu.VMEM((n_high // 2, blocks, part, lanes), f32),
            pltpu.VMEM((n_high // 2, blocks, part, lanes), f32),
            pltpu.SemaphoreType.DMA((2,)),
            pltpu.SemaphoreType.DMA((5,)),
            pltpu.SemaphoreType.DMA((chunks, count)),
            pltpu.SemaphoreType.DMA((chunks, count)),
            pltpu.SemaphoreType.DMA((chunks, count)),
            pltpu.SemaphoreType.DMA((n_high // 2,)),
            pltpu.SemaphoreType.DMA((n_high // 2,)),
        ],
        compiler_params=pltpu.CompilerParams(collective_id=0, has_side_effects=True),
    )(mix_angles, wave_parts, level_table, phase_angles)
    result, marginal = pl.pallas_call(
        finish,
        out_shape=[
            jax.ShapeDtypeStruct(wave_parts.shape, f32),
            jax.ShapeDtypeStruct((blocks, part, lanes), f32),
        ],
        in_specs=[vmem, vmem],
        out_specs=[any_space, any_space],
        scratch_shapes=[pltpu.SemaphoreType.DMA((2,))],
    )(*(pltpu.with_memory_space_constraint(x, pltpu.VMEM) for x in (back, total)))
    return (result, marginal)


def solution(mesh):
    in_specs = (P(None, ("high", "low"), None, None), P(("high", "low"), None, None), P(), P())
    out_specs = (P(None, ("high", "low"), None, None), P("low", "high", None))
    return jax.shard_map(
        functools.partial(on_device, mesh.shape["high"], mesh.shape["low"]),
        mesh=mesh, in_specs=in_specs, out_specs=out_specs, check_vma=False,
    )
```

```python
import functools

import jax
import jax.numpy as jnp
from jax import lax
from jax.experimental import pallas as pl
from jax.experimental.pallas import tpu as pltpu
from jax.sharding import PartitionSpec as P

LAYERS = 2
MESH = pl.DeviceIdType.MESH
SUBLANES = 8
TERMS = 5


def count_bits(values, count):
    places = jnp.arange(count.bit_length() - 1, dtype=jnp.int32)
    return jnp.sum(values[..., None] >> places & 1, axis=-1)


def real_turn_table(count, angle):
    rank = jnp.arange(count, dtype=jnp.int32)
    apart = count_bits(rank[:, None] ^ rank[None, :], count)
    minus = count_bits(rank[:, None] & (rank[:, None] ^ rank[None, :]), count)
    bits = count.bit_length() - 1
    size = jnp.cos(angle) ** (bits - apart).astype(jnp.float32) * jnp.sin(angle) ** apart.astype(
        jnp.float32
    )
    return size * jnp.where(minus % 2 == 1, -1.0, 1.0).astype(jnp.float32)


def apply_along(values, dim, angle):
    real_part = real_turn_table(values.shape[dim], angle)
    moved = jnp.tensordot(values, real_part, axes=([dim], [0]), precision=lax.Precision.HIGHEST)
    return jnp.moveaxis(moved, -1, dim)


def phase_step(values, levels, angle):
    turn = angle * levels
    return jnp.stack(
        [
            values[0] * jnp.cos(turn) + values[1] * jnp.sin(turn),
            values[1] * jnp.cos(turn) - values[0] * jnp.sin(turn),
        ]
    )


def by_axis(wave_parts, level_table, phase_angles, mix_angles):
    values = wave_parts
    for layer in range(LAYERS):
        values = phase_step(values, level_table, phase_angles[layer])
        values = apply_along(values, 3, mix_angles[layer, 0])
        values = apply_along(values, 2, mix_angles[layer, 1])
        values = apply_along(values, 1, mix_angles[layer, 2])
        moved = lax.all_to_all(values, "high", split_axis=2, concat_axis=1, tiled=True)
        spread = moved.reshape(2, lax.axis_size("high"), -1, moved.shape[2], moved.shape[3])
        moved = apply_along(spread, 1, mix_angles[layer, 2]).reshape(moved.shape)
        values = lax.all_to_all(moved, "high", split_axis=1, concat_axis=2, tiled=True)
        moved = lax.all_to_all(values, "low", split_axis=3, concat_axis=1, tiled=True)
        spread = moved.reshape(2, lax.axis_size("low"), -1, moved.shape[2], moved.shape[3])
        moved = apply_along(spread, 1, mix_angles[layer, 3]).reshape(moved.shape)
        values = lax.all_to_all(moved, "low", split_axis=1, concat_axis=3, tiled=True)
    chance = values[0] * values[0] + values[1] * values[1]
    marginal = lax.psum_scatter(chance, "high", scatter_dimension=1, tiled=True) / lax.axis_size(
        "high"
    )
    return (values, marginal)


def mix_list(values, groups):
    values = list(values)
    stride = 1
    for bits, cos, sin in groups:
        for _ in range(bits):
            for at in range(len(values)):
                if at & stride == 0:
                    u, v = values[at], values[at + stride]
                    values[at] = cos * u - sin * v
                    values[at + stride] = cos * v + sin * u
            stride *= 2
    return values


def series(square, first):
    terms = [1.0]
    for n in range(TERMS):
        terms.append(-terms[-1] / ((2 * n + first) * (2 * n + first + 1)))
    out = jnp.full_like(square, terms[-1])
    for term in terms[-2::-1]:
        out = out * square + term
    return out


def cos_sin(half):
    square = half * half
    cos, sin = series(square, 1), half * series(square, 2)
    twice = sin + sin
    return 1.0 - twice * sin, twice * cos


def turn_matrix(groups, sign):
    size = 1
    for bits, _, _ in groups:
        size <<= bits
    row = lax.broadcasted_iota(jnp.int32, (size, size), 0)
    column = lax.broadcasted_iota(jnp.int32, (size, size), 1)
    out = None
    place = 0
    for bits, cos, sin in groups:
        up = sign * sin
        for _ in range(bits):
            kb = (row >> place) & 1
            nb = (column >> place) & 1
            factor = jnp.where(kb == nb, cos, jnp.where(nb > kb, up, -up))
            out = factor if out is None else out * factor
            place += 1
    return out


def split(values):
    high = values.astype(jnp.bfloat16)
    return high, (values - high.astype(jnp.float32)).astype(jnp.bfloat16)


def dot(left, right):
    return jnp.dot(left, right, preferred_element_type=jnp.float32)


def doublings(first, end):
    return [1 << i for i in range(first.bit_length() - 1, end.bit_length() - 1)]


def log2(count):
    return count.bit_length() - 1


def turn_chunks(ref, t, h, part, pair):
    chunks = part // SUBLANES
    at = [pl.ds(h * part + j * SUBLANES, SUBLANES) for j in range(chunks)]
    return [mix_list([ref[p, t, r, :] for r in at], [(log2(chunks), *pair)]) for p in range(2)]


def finish(back, total, out_hbm, marginal_hbm, sem):
    copies = [
        pltpu.make_async_copy(back, out_hbm, sem.at[0]),
        pltpu.make_async_copy(total, marginal_hbm, sem.at[1]),
    ]
    for copy in copies:
        copy.start()
    for copy in copies:
        copy.wait()


def kernel(
    n_high, n_low,
    mix_ref, wave_hbm, level_hbm, phase_ref,
    back, total,
    wave_ref, level_ref, level_far, a_ref, b_ref, c_ref, level_b, chance, pair, sums, gathered,
    ready, load_sem, send_sem, recv_far, recv_state, recv_level, recv_back, recv_pair, recv_sums,
):
    loads = [
        pltpu.make_async_copy(level_hbm, level_ref, load_sem.at[0]),
        pltpu.make_async_copy(wave_hbm, wave_ref, load_sem.at[1]),
    ]
    for load in loads:
        load.start()
    _, blocks, rows, lanes = wave_ref.shape
    part = rows // n_high
    chunks = part // SUBLANES
    count = n_high * n_low
    twos = half = n_high // 2
    mh, ml = lax.axis_index("high"), lax.axis_index("low")

    barrier = pltpu.get_barrier_semaphore()

    def other(i):
        k = 1 + i
        return k, (mh + k // n_low) % n_high, (ml + k % n_low) % n_low

    def flip(value, bit):
        return value + bit * (1 - 2 * (value // bit % 2))

    mz, mc = mh // 2, mh % 2
    far = (mh + half) % n_high
    mine = mh // half * half

    @pl.loop(1, 2 * n_low)
    def _(i):
        dh, dl = mz * 2 + (mc + i // n_low) % 2, (ml + i % n_low) % n_low
        pl.semaphore_signal(barrier, inc=1, device_id=(dh, dl), device_id_type=MESH)

    for bit in doublings(2, n_high):
        pl.semaphore_signal(barrier, inc=1, device_id=(flip(mh, bit), ml), device_id_type=MESH)

    def angles(layer, group):
        angle = jnp.full((SUBLANES, lanes), mix_ref[layer, group], jnp.float32)
        return jnp.cos(angle), jnp.sin(angle)

    def wide(pair, size):
        return tuple(jnp.broadcast_to(x[:1, :1], (size, size)) for x in pair)

    def phase(re, im, levels, layer):
        cos, sin = cos_sin(phase_ref[pl.ds(layer, 1), :] * 0.5 * levels)
        return re * cos + im * sin, im * cos - re * sin

    def tile(h, j):
        return pl.ds(pl.multiple_of(h * part + j * SUBLANES, SUBLANES), SUBLANES)

    def rows_of(h):
        return pl.ds(pl.multiple_of(h * part, SUBLANES), part)

    def mix_in_a(ref, j, layer):
        row_pair, block_pair = angles(layer, 1), angles(layer, 2)
        groups = [(log2(n_high), *row_pair), (log2(blocks), *block_pair)]
        at = [(t, tile(h, j)) for t in range(blocks) for h in range(n_high)]
        for p in range(2):
            values = mix_list([ref[p, t, r, :] for t, r in at], groups)
            for (t, r), value in zip(at, values):
                ref[p, t, r, :] = value

    def mix_chunks(ref, t, h, layer):
        return turn_chunks(ref, t, h, part, angles(layer, 1))

    def tables(layer):
        lane = split(turn_matrix([(log2(lanes), *wide(angles(layer, 0), lanes))], 1.0))
        packed = jnp.concatenate(
            [jnp.concatenate(lane, axis=1), jnp.concatenate([lane[0], jnp.zeros_like(lane[0])], axis=1)], axis=0
        )
        size = count * SUBLANES
        row_pair, block_pair, low_pair = (wide(angles(layer, g), size) for g in (1, 2, 3))
        upper = turn_matrix(
            [(log2(SUBLANES), *row_pair), (log2(n_high), *block_pair), (log2(n_low), *low_pair)], -1.0
        )
        return packed, split(upper)

    def mix_in_b(ref, j, packed, upper):
        size = count * SUBLANES
        both = jnp.concatenate([ref[j, p].reshape(size, lanes) for p in range(2)], axis=1)
        high, low = split(both)
        both = dot(upper[0], high) + (dot(upper[1], high) + dot(upper[0], low))
        rows = jnp.concatenate([both[:, :lanes], both[:, lanes:]], axis=0)
        out = dot(jnp.concatenate(split(rows), axis=1), packed)
        out = out[:, :lanes] + out[:, lanes:]
        for p in range(2):
            c_ref[j, p] = out[p * size : (p + 1) * size].reshape(n_low, n_high, SUBLANES, lanes)

    def state_copy(j, i):
        k, dh, dl = other(i)
        return pltpu.make_async_remote_copy(
            src_ref=a_ref.at[:, dl, tile(dh, j), :],
            dst_ref=b_ref.at[j, :, ml, mh],
            send_sem=send_sem.at[0],
            recv_sem=recv_state.at[j, k],
            device_id=(dh, dl),
            device_id_type=MESH,
        )

    def far_copy(t):
        return pltpu.make_async_remote_copy(
            src_ref=level_ref.at[t, pl.ds(pl.multiple_of((half - mine) * part, SUBLANES), half * part), :],
            dst_ref=level_far.at[t],
            send_sem=send_sem.at[5],
            recv_sem=recv_far.at[t],
            device_id=(far, ml),
            device_id_type=MESH,
        )

    def level_copy(whose, i):
        k = 1 + i
        dh, dl = (mh - mine + k // n_low) % half, (ml + k % n_low) % n_low
        return pltpu.make_async_remote_copy(
            src_ref=[level_ref.at[dl, rows_of(mine + dh), :], level_far.at[dl, rows_of(dh), :]][whose],
            dst_ref=level_b.at[ml, [mh, far][whose]],
            send_sem=send_sem.at[1],
            recv_sem=recv_level.at[whose, k],
            device_id=(mine + dh, dl),
            device_id_type=MESH,
        )

    def back_copy(j, i):
        k, dh, dl = other(i)
        return pltpu.make_async_remote_copy(
            src_ref=c_ref.at[j, :, dl, dh],
            dst_ref=back.at[:, ml, tile(mh, j), :],
            send_sem=send_sem.at[2],
            recv_sem=recv_back.at[j, k],
            device_id=(dh, dl),
            device_id_type=MESH,
        )

    def each(do, copy, j):
        @pl.loop(0, half * n_low - 1 if copy is level_copy else count - 1)
        def _(i):
            getattr(copy(j, i), do)()

    bits = doublings(2, n_high)

    def tell(i):
        pl.semaphore_signal(ready.at[i], inc=1, device_id=(flip(mh, bits[i]), ml), device_id_type=MESH)

    def hear(i):
        pl.semaphore_wait(ready.at[i], 1)

    loads[0].wait()
    pl.semaphore_wait(barrier, 2 * n_low - 1 + len(bits))
    for t in range(blocks):
        far_copy(t).start()
    tell(0)
    loads[1].wait()

    @pl.loop(0, blocks * rows // 32)
    def _(i):
        t, r = i // (rows // 32), pl.ds(pl.multiple_of(i % (rows // 32) * 32, 32), 32)
        re, im = phase(wave_ref[0, t, r, :], wave_ref[1, t, r, :], level_ref[t, r, :], 0)
        a_ref[0, t, r, :] = re
        a_ref[1, t, r, :] = im

    for i in range(1, len(bits)):
        hear(i - 1)
        tell(i)

    @pl.loop(0, chunks)
    def _(j):
        mix_in_a(a_ref, j, 0)

    @pl.loop(0, blocks)
    def _(t):
        for h in range(n_high):
            for p, values in enumerate(mix_chunks(a_ref, t, h, 0)):
                for j, value in enumerate(values):
                    a_ref[p, t, tile(h, j), :] = value

    hear(len(bits) - 1)
    each("start", state_copy, 0)
    each("start", level_copy, 0)
    first, second = tables(0), tables(1)
    for j in range(chunks):
        b_ref[j, :, ml, mh] = a_ref[:, ml, tile(mh, j), :]
    level_b[ml, mh] = level_ref[ml, rows_of(mh), :]
    for t in range(blocks):
        far_copy(t).wait_recv()
    each("start", level_copy, 1)
    for j in range(1, chunks):
        each("start", state_copy, j)
    level_b[ml, far] = level_far[ml, rows_of(mh - mine), :]

    for j in range(chunks):
        each("wait_recv", state_copy, j)
        mix_in_b(b_ref, j, *first)
        if j == 0:
            each("wait_recv", level_copy, 0)
            each("wait_recv", level_copy, 1)

        @pl.loop(0, n_low)
        def _(l):
            levels = level_b[l, :, j * SUBLANES : (j + 1) * SUBLANES, :]
            re, im = phase(c_ref[j, 0, l], c_ref[j, 1, l], levels, 1)
            c_ref[j, 0, l] = re
            c_ref[j, 1, l] = im

        mix_in_b(c_ref, j, *second)
        each("start", back_copy, j)
        back[:, ml, tile(mh, j), :] = c_ref[j, :, ml, mh]

    for j in range(chunks):
        each("wait_recv", back_copy, j)
        mix_in_a(back, j, 1)

    @pl.loop(0, blocks)
    def _(t):
        for h in range(n_high):
            re, im = mix_chunks(back, t, h, 1)
            for j in range(chunks):
                back[0, t, tile(h, j), :] = re[j]
                back[1, t, tile(h, j), :] = im[j]
                chance[h % 2, h // 2, t, pl.ds(j * SUBLANES, SUBLANES), :] = re[j] * re[j] + im[j] * im[j]

    def pair_copy(i):
        dz = (mz + i + 1) % twos
        return dz, pltpu.make_async_remote_copy(
            src_ref=chance.at[1 - mc, dz],
            dst_ref=pair.at[dz],
            send_sem=send_sem.at[3],
            recv_sem=recv_pair.at[i],
            device_id=(mz * 2 + 1 - mc, ml),
            device_id_type=MESH,
        )

    def sums_copy(i):
        dz = (mz + i + 1) % twos
        return pltpu.make_async_remote_copy(
            src_ref=sums.at[dz],
            dst_ref=gathered.at[mz],
            send_sem=send_sem.at[4],
            recv_sem=recv_sums.at[i],
            device_id=(dz * 2 + mc, ml),
            device_id_type=MESH,
        )

    for i in range(twos):
        pair_copy(i)[1].start()
    for i in range(twos):
        dz, copy = pair_copy(i)
        copy.wait_recv()
        summed = chance[mc, dz] + pair[dz]
        if i < twos - 1:
            sums[dz] = summed
            sums_copy(i).start()
        else:
            gathered[dz] = summed
    for i in range(twos - 1):
        sums_copy(i).wait_recv()
    summed = gathered[0]
    for z in range(1, twos):
        summed = summed + gathered[z]
    total[...] = summed * (1.0 / n_high)
    for j in range(chunks):
        each("wait_send", state_copy, j)
        each("wait_send", back_copy, j)
    for whose in range(2):
        each("wait_send", level_copy, whose)
    for t in range(blocks):
        far_copy(t).wait_send()
    for i in range(twos):
        pair_copy(i)[1].wait_send()
    for i in range(twos - 1):
        sums_copy(i).wait_send()


def on_device(n_high, n_low, wave_parts, level_table, phase_angles, mix_angles):
    _, blocks, rows, lanes = wave_parts.shape
    if blocks != n_low or n_high < 4 or n_high & (n_high - 1) or rows % (n_high * SUBLANES):
        return by_axis(wave_parts, level_table, phase_angles, mix_angles)
    part = rows // n_high
    chunks = part // SUBLANES
    count = n_high * n_low
    f32 = jnp.float32
    vmem = pl.BlockSpec(memory_space=pltpu.VMEM)
    any_space = pl.BlockSpec(memory_space=pl.ANY)
    smem = pl.BlockSpec(memory_space=pltpu.SMEM)
    back, total = pl.pallas_call(
        functools.partial(kernel, n_high, n_low),
        out_shape=[
            pltpu.VMEM(wave_parts.shape, f32),
            pltpu.VMEM((blocks, part, lanes), f32),
        ],
        in_specs=[smem, any_space, any_space, vmem],
        out_specs=[vmem, vmem],
        scratch_shapes=[
            pltpu.VMEM((2, blocks, rows, lanes), f32),
            pltpu.VMEM((blocks, rows, lanes), f32),
            pltpu.VMEM((blocks, rows // 2, lanes), f32),
            pltpu.VMEM((2, blocks, rows, lanes), f32),
            pltpu.VMEM((chunks, 2, n_low, n_high, SUBLANES, lanes), f32),
            pltpu.VMEM((chunks, 2, n_low, n_high, SUBLANES, lanes), f32),
            pltpu.VMEM((n_low, n_high, part, lanes), f32),
            pltpu.VMEM((2, n_high // 2, blocks, part, lanes), f32),
            pltpu.VMEM((n_high // 2, blocks, part, lanes), f32),
            pltpu.VMEM((n_high // 2, blocks, part, lanes), f32),
            pltpu.VMEM((n_high // 2, blocks, part, lanes), f32),
            pltpu.SemaphoreType.REGULAR((log2(n_high) - 1,)),
            pltpu.SemaphoreType.DMA((2,)),
            pltpu.SemaphoreType.DMA((6,)),
            pltpu.SemaphoreType.DMA((blocks,)),
            pltpu.SemaphoreType.DMA((chunks, count)),
            pltpu.SemaphoreType.DMA((2, count // 2)),
            pltpu.SemaphoreType.DMA((chunks, count)),
            pltpu.SemaphoreType.DMA((n_high // 2,)),
            pltpu.SemaphoreType.DMA((n_high // 2,)),
        ],
        compiler_params=pltpu.CompilerParams(collective_id=0, has_side_effects=True),
    )(mix_angles, wave_parts, level_table, phase_angles)
    result, marginal = pl.pallas_call(
        finish,
        out_shape=[
            jax.ShapeDtypeStruct(wave_parts.shape, f32),
            jax.ShapeDtypeStruct((blocks, part, lanes), f32),
        ],
        in_specs=[vmem, vmem],
        out_specs=[any_space, any_space],
        scratch_shapes=[pltpu.SemaphoreType.DMA((2,))],
    )(*(pltpu.with_memory_space_constraint(x, pltpu.VMEM) for x in (back, total)))
    return (result, marginal)


def solution(mesh):
    in_specs = (P(None, ("high", "low"), None, None), P(("high", "low"), None, None), P(), P())
    out_specs = (P(None, ("high", "low"), None, None), P("low", "high", None))
    return jax.shard_map(
        functools.partial(on_device, mesh.shape["high"], mesh.shape["low"]),
        mesh=mesh, in_specs=in_specs, out_specs=out_specs, check_vma=False,
    )
```

```python
import functools

import jax
import jax.numpy as jnp
from jax import lax
from jax.experimental import pallas as pl
from jax.experimental.pallas import tpu as pltpu
from jax.sharding import PartitionSpec as P

LAYERS = 2
MESH = pl.DeviceIdType.MESH
SUBLANES = 8
TERMS = 5


def count_bits(values, count):
    places = jnp.arange(count.bit_length() - 1, dtype=jnp.int32)
    return jnp.sum(values[..., None] >> places & 1, axis=-1)


def real_turn_table(count, angle):
    rank = jnp.arange(count, dtype=jnp.int32)
    apart = count_bits(rank[:, None] ^ rank[None, :], count)
    minus = count_bits(rank[:, None] & (rank[:, None] ^ rank[None, :]), count)
    bits = count.bit_length() - 1
    size = jnp.cos(angle) ** (bits - apart).astype(jnp.float32) * jnp.sin(angle) ** apart.astype(
        jnp.float32
    )
    return size * jnp.where(minus % 2 == 1, -1.0, 1.0).astype(jnp.float32)


def apply_along(values, dim, angle):
    real_part = real_turn_table(values.shape[dim], angle)
    moved = jnp.tensordot(values, real_part, axes=([dim], [0]), precision=lax.Precision.HIGHEST)
    return jnp.moveaxis(moved, -1, dim)


def phase_step(values, levels, angle):
    turn = angle * levels
    return jnp.stack(
        [
            values[0] * jnp.cos(turn) + values[1] * jnp.sin(turn),
            values[1] * jnp.cos(turn) - values[0] * jnp.sin(turn),
        ]
    )


def by_axis(wave_parts, level_table, phase_angles, mix_angles):
    values = wave_parts
    for layer in range(LAYERS):
        values = phase_step(values, level_table, phase_angles[layer])
        values = apply_along(values, 3, mix_angles[layer, 0])
        values = apply_along(values, 2, mix_angles[layer, 1])
        values = apply_along(values, 1, mix_angles[layer, 2])
        moved = lax.all_to_all(values, "high", split_axis=2, concat_axis=1, tiled=True)
        spread = moved.reshape(2, lax.axis_size("high"), -1, moved.shape[2], moved.shape[3])
        moved = apply_along(spread, 1, mix_angles[layer, 2]).reshape(moved.shape)
        values = lax.all_to_all(moved, "high", split_axis=1, concat_axis=2, tiled=True)
        moved = lax.all_to_all(values, "low", split_axis=3, concat_axis=1, tiled=True)
        spread = moved.reshape(2, lax.axis_size("low"), -1, moved.shape[2], moved.shape[3])
        moved = apply_along(spread, 1, mix_angles[layer, 3]).reshape(moved.shape)
        values = lax.all_to_all(moved, "low", split_axis=1, concat_axis=3, tiled=True)
    chance = values[0] * values[0] + values[1] * values[1]
    marginal = lax.psum_scatter(chance, "high", scatter_dimension=1, tiled=True) / lax.axis_size(
        "high"
    )
    return (values, marginal)


def mix_list(values, groups):
    values = list(values)
    stride = 1
    for bits, cos, sin in groups:
        for _ in range(bits):
            for at in range(len(values)):
                if at & stride == 0:
                    u, v = values[at], values[at + stride]
                    values[at] = cos * u - sin * v
                    values[at + stride] = cos * v + sin * u
            stride *= 2
    return values


def series(square, first):
    terms = [1.0]
    for n in range(TERMS):
        terms.append(-terms[-1] / ((2 * n + first) * (2 * n + first + 1)))
    out = jnp.full_like(square, terms[-1])
    for term in terms[-2::-1]:
        out = out * square + term
    return out


def cos_sin(half):
    square = half * half
    cos, sin = series(square, 1), half * series(square, 2)
    twice = sin + sin
    return 1.0 - twice * sin, twice * cos


def turn_matrix(groups, sign):
    size = 1
    for bits, _, _ in groups:
        size <<= bits
    row = lax.broadcasted_iota(jnp.int32, (size, size), 0)
    column = lax.broadcasted_iota(jnp.int32, (size, size), 1)
    out = None
    place = 0
    for bits, cos, sin in groups:
        up = sign * sin
        for _ in range(bits):
            kb = (row >> place) & 1
            nb = (column >> place) & 1
            factor = jnp.where(kb == nb, cos, jnp.where(nb > kb, up, -up))
            out = factor if out is None else out * factor
            place += 1
    return out


def split(values):
    high = values.astype(jnp.bfloat16)
    return high, (values - high.astype(jnp.float32)).astype(jnp.bfloat16)


def dot(left, right):
    return jnp.dot(left, right, preferred_element_type=jnp.float32)


def spread(count):
    even, odd = list(range(2, count, 2)), list(range(1, count, 2))
    middle = len(even) // 2
    return even[:middle] + even[middle + 1 :] + even[middle : middle + 1] + odd + [0]


def doublings(first, end):
    return [1 << i for i in range(first.bit_length() - 1, end.bit_length() - 1)]


def log2(count):
    return count.bit_length() - 1


def turn_chunks(ref, t, h, part, pair):
    chunks = part // SUBLANES
    at = [pl.ds(h * part + j * SUBLANES, SUBLANES) for j in range(chunks)]
    return [mix_list([ref[p, t, r, :] for r in at], [(log2(chunks), *pair)]) for p in range(2)]


def finish(back, total, out_hbm, marginal_hbm, sem):
    copies = [
        pltpu.make_async_copy(back, out_hbm, sem.at[0]),
        pltpu.make_async_copy(total, marginal_hbm, sem.at[1]),
    ]
    for copy in copies:
        copy.start()
    for copy in copies:
        copy.wait()


def kernel(
    n_high, n_low,
    mix_ref, wave_hbm, level_hbm, phase_ref,
    back, total,
    wave_ref, level_ref, level_far, a_ref, b_ref, c_ref, level_b, chance, pair, sums, gathered,
    ready, load_sem, send_sem, recv_far, recv_state, recv_level, recv_back, recv_pair, recv_sums,
):
    loads = [
        pltpu.make_async_copy(level_hbm, level_ref, load_sem.at[0]),
        pltpu.make_async_copy(wave_hbm, wave_ref, load_sem.at[1]),
    ]
    for load in loads:
        load.start()
    _, blocks, rows, lanes = wave_ref.shape
    part = rows // n_high
    chunks = part // SUBLANES
    count = n_high * n_low
    twos = half = n_high // 2
    mh, ml = lax.axis_index("high"), lax.axis_index("low")

    barrier = pltpu.get_barrier_semaphore()

    def other(i):
        k = 1 + i
        return k, (mh + k // n_low) % n_high, (ml + k % n_low) % n_low

    def flip(value, bit):
        return value + bit * (1 - 2 * (value // bit % 2))

    mz, mc = mh // 2, mh % 2
    far = (mh + half) % n_high
    mine = mh // half * half

    @pl.loop(1, 2 * n_low)
    def _(i):
        dh, dl = mz * 2 + (mc + i // n_low) % 2, (ml + i % n_low) % n_low
        pl.semaphore_signal(barrier, inc=1, device_id=(dh, dl), device_id_type=MESH)

    for bit in doublings(2, n_high):
        pl.semaphore_signal(barrier, inc=1, device_id=(flip(mh, bit), ml), device_id_type=MESH)

    def angles(layer, group):
        angle = jnp.full((SUBLANES, lanes), mix_ref[layer, group], jnp.float32)
        return jnp.cos(angle), jnp.sin(angle)

    def wide(pair, size):
        return tuple(jnp.broadcast_to(x[:1, :1], (size, size)) for x in pair)

    def phase(re, im, levels, layer):
        cos, sin = cos_sin(phase_ref[pl.ds(layer, 1), :] * 0.5 * levels)
        return re * cos + im * sin, im * cos - re * sin

    def tile(h, j):
        return pl.ds(pl.multiple_of(h * part + j * SUBLANES, SUBLANES), SUBLANES)

    def rows_of(h):
        return pl.ds(pl.multiple_of(h * part, SUBLANES), part)

    def mix_in_a(ref, j, layer):
        row_pair, block_pair = angles(layer, 1), angles(layer, 2)
        groups = [(log2(n_high), *row_pair), (log2(blocks), *block_pair)]
        at = [(t, tile(h, j)) for t in range(blocks) for h in range(n_high)]
        for p in range(2):
            values = mix_list([ref[p, t, r, :] for t, r in at], groups)
            for (t, r), value in zip(at, values):
                ref[p, t, r, :] = value

    def mix_chunks(ref, t, h, layer):
        return turn_chunks(ref, t, h, part, angles(layer, 1))

    def tables(layer):
        lane = split(turn_matrix([(log2(lanes), *wide(angles(layer, 0), lanes))], 1.0))
        packed = jnp.concatenate(
            [jnp.concatenate(lane, axis=1), jnp.concatenate([lane[0], jnp.zeros_like(lane[0])], axis=1)], axis=0
        )
        size = count * SUBLANES
        row_pair, block_pair, low_pair = (wide(angles(layer, g), size) for g in (1, 2, 3))
        upper = turn_matrix(
            [(log2(SUBLANES), *row_pair), (log2(n_high), *block_pair), (log2(n_low), *low_pair)], -1.0
        )
        return packed, split(upper)

    def mix_in_b(ref, j, packed, upper):
        size = count * SUBLANES
        both = jnp.concatenate([ref[j, p].reshape(size, lanes) for p in range(2)], axis=1)
        high, low = split(both)
        both = dot(upper[0], high) + (dot(upper[1], high) + dot(upper[0], low))
        rows = jnp.concatenate([both[:, :lanes], both[:, lanes:]], axis=0)
        out = dot(jnp.concatenate(split(rows), axis=1), packed)
        out = out[:, :lanes] + out[:, lanes:]
        for p in range(2):
            c_ref[j, p] = out[p * size : (p + 1) * size].reshape(n_low, n_high, SUBLANES, lanes)

    def state_copy(j, i):
        k, dh, dl = other(i)
        return pltpu.make_async_remote_copy(
            src_ref=a_ref.at[:, dl, tile(dh, j), :],
            dst_ref=b_ref.at[j, :, ml, mh],
            send_sem=send_sem.at[0],
            recv_sem=recv_state.at[j, k],
            device_id=(dh, dl),
            device_id_type=MESH,
        )

    def far_copy(t):
        return pltpu.make_async_remote_copy(
            src_ref=level_ref.at[t, pl.ds(pl.multiple_of((half - mine) * part, SUBLANES), half * part), :],
            dst_ref=level_far.at[t],
            send_sem=send_sem.at[5],
            recv_sem=recv_far.at[t],
            device_id=(far, ml),
            device_id_type=MESH,
        )

    def level_copy(whose, i):
        k = 1 + i
        dh, dl = (mh - mine + k // n_low) % half, (ml + k % n_low) % n_low
        return pltpu.make_async_remote_copy(
            src_ref=[level_ref.at[dl, rows_of(mine + dh), :], level_far.at[dl, rows_of(dh), :]][whose],
            dst_ref=level_b.at[ml, [mh, far][whose]],
            send_sem=send_sem.at[1],
            recv_sem=recv_level.at[whose, k],
            device_id=(mine + dh, dl),
            device_id_type=MESH,
        )

    def back_copy(j, i):
        k, dh, dl = other(i)
        return pltpu.make_async_remote_copy(
            src_ref=c_ref.at[j, :, dl, dh],
            dst_ref=back.at[:, ml, tile(mh, j), :],
            send_sem=send_sem.at[2],
            recv_sem=recv_back.at[j, k],
            device_id=(dh, dl),
            device_id_type=MESH,
        )

    def each(do, copy, j):
        planes = range(half) if copy is level_copy else spread(n_high)
        for i in [h * n_low + l - 1 for h in planes for l in range(n_low) if h or l]:
            getattr(copy(j, i), do)()

    bits = doublings(2, n_high)

    def tell(i):
        pl.semaphore_signal(ready.at[i], inc=1, device_id=(flip(mh, bits[i]), ml), device_id_type=MESH)

    def hear(i):
        pl.semaphore_wait(ready.at[i], 1)

    loads[0].wait()
    pl.semaphore_wait(barrier, 2 * n_low - 1 + len(bits))
    for t in range(blocks):
        far_copy(t).start()
    tell(0)
    loads[1].wait()

    @pl.loop(0, blocks * rows // 32)
    def _(i):
        t, r = i // (rows // 32), pl.ds(pl.multiple_of(i % (rows // 32) * 32, 32), 32)
        re, im = phase(wave_ref[0, t, r, :], wave_ref[1, t, r, :], level_ref[t, r, :], 0)
        a_ref[0, t, r, :] = re
        a_ref[1, t, r, :] = im

    for i in range(1, len(bits)):
        hear(i - 1)
        tell(i)

    @pl.loop(0, chunks)
    def _(j):
        mix_in_a(a_ref, j, 0)

    @pl.loop(0, blocks)
    def _(t):
        for h in range(n_high):
            for p, values in enumerate(mix_chunks(a_ref, t, h, 0)):
                for j, value in enumerate(values):
                    a_ref[p, t, tile(h, j), :] = value

    hear(len(bits) - 1)
    each("start", state_copy, 0)
    each("start", level_copy, 0)
    first, second = tables(0), tables(1)
    for j in range(chunks):
        b_ref[j, :, ml, mh] = a_ref[:, ml, tile(mh, j), :]
    level_b[ml, mh] = level_ref[ml, rows_of(mh), :]
    for t in range(blocks):
        far_copy(t).wait_recv()
    each("start", level_copy, 1)
    for j in range(1, chunks):
        each("start", state_copy, j)
    level_b[ml, far] = level_far[ml, rows_of(mh - mine), :]

    for j in range(chunks):
        each("wait_recv", state_copy, j)
        mix_in_b(b_ref, j, *first)
        if j == 0:
            each("wait_recv", level_copy, 0)
            each("wait_recv", level_copy, 1)

        @pl.loop(0, n_low)
        def _(l):
            levels = level_b[l, :, j * SUBLANES : (j + 1) * SUBLANES, :]
            re, im = phase(c_ref[j, 0, l], c_ref[j, 1, l], levels, 1)
            c_ref[j, 0, l] = re
            c_ref[j, 1, l] = im

        mix_in_b(c_ref, j, *second)
        each("start", back_copy, j)
        back[:, ml, tile(mh, j), :] = c_ref[j, :, ml, mh]

    for j in range(chunks):
        each("wait_send", state_copy, j)
    for whose in range(2):
        each("wait_send", level_copy, whose)
    for t in range(blocks):
        far_copy(t).wait_send()

    for j in range(chunks):
        each("wait_recv", back_copy, j)
        mix_in_a(back, j, 1)

    @pl.loop(0, blocks)
    def _(t):
        for h in range(n_high):
            re, im = mix_chunks(back, t, h, 1)
            for j in range(chunks):
                back[0, t, tile(h, j), :] = re[j]
                back[1, t, tile(h, j), :] = im[j]
                chance[h % 2, h // 2, t, pl.ds(j * SUBLANES, SUBLANES), :] = re[j] * re[j] + im[j] * im[j]

    def pair_copy(i):
        dz = (mz + i + 1) % twos
        return dz, pltpu.make_async_remote_copy(
            src_ref=chance.at[mc, dz],
            dst_ref=pair.at[dz],
            send_sem=send_sem.at[3],
            recv_sem=recv_pair.at[i],
            device_id=(mz * 2 + 1 - mc, ml),
            device_id_type=MESH,
        )

    def sums_copy(i):
        dz = (mz + i + 1) % twos
        return pltpu.make_async_remote_copy(
            src_ref=sums.at[dz],
            dst_ref=gathered.at[mz],
            send_sem=send_sem.at[4],
            recv_sem=recv_sums.at[i],
            device_id=(dz * 2 + 1 - mc, ml),
            device_id_type=MESH,
        )

    for i in range(twos):
        pair_copy(i)[1].start()
    for i in range(twos):
        dz, copy = pair_copy(i)
        copy.wait_recv()
        sums[dz] = chance[1 - mc, dz] + pair[dz]
        sums_copy(i).start()
    for j in range(chunks):
        each("wait_send", back_copy, j)
    for i in range(twos):
        pair_copy(i)[1].wait_send()
    for i in range(twos):
        sums_copy(i).wait_recv()
    summed = gathered[0]
    for z in range(1, twos):
        summed = summed + gathered[z]
    total[...] = summed * (1.0 / n_high)
    for i in range(twos):
        sums_copy(i).wait_send()


def on_device(n_high, n_low, wave_parts, level_table, phase_angles, mix_angles):
    _, blocks, rows, lanes = wave_parts.shape
    if blocks != n_low or n_high < 4 or n_high & (n_high - 1) or rows % (n_high * SUBLANES):
        return by_axis(wave_parts, level_table, phase_angles, mix_angles)
    part = rows // n_high
    chunks = part // SUBLANES
    count = n_high * n_low
    f32 = jnp.float32
    vmem = pl.BlockSpec(memory_space=pltpu.VMEM)
    any_space = pl.BlockSpec(memory_space=pl.ANY)
    smem = pl.BlockSpec(memory_space=pltpu.SMEM)
    back, total = pl.pallas_call(
        functools.partial(kernel, n_high, n_low),
        out_shape=[
            pltpu.VMEM(wave_parts.shape, f32),
            pltpu.VMEM((blocks, part, lanes), f32),
        ],
        in_specs=[smem, any_space, any_space, vmem],
        out_specs=[vmem, vmem],
        scratch_shapes=[
            pltpu.VMEM((2, blocks, rows, lanes), f32),
            pltpu.VMEM((blocks, rows, lanes), f32),
            pltpu.VMEM((blocks, rows // 2, lanes), f32),
            pltpu.VMEM((2, blocks, rows, lanes), f32),
            pltpu.VMEM((chunks, 2, n_low, n_high, SUBLANES, lanes), f32),
            pltpu.VMEM((chunks, 2, n_low, n_high, SUBLANES, lanes), f32),
            pltpu.VMEM((n_low, n_high, part, lanes), f32),
            pltpu.VMEM((2, n_high // 2, blocks, part, lanes), f32),
            pltpu.VMEM((n_high // 2, blocks, part, lanes), f32),
            pltpu.VMEM((n_high // 2, blocks, part, lanes), f32),
            pltpu.VMEM((n_high // 2, blocks, part, lanes), f32),
            pltpu.SemaphoreType.REGULAR((log2(n_high) - 1,)),
            pltpu.SemaphoreType.DMA((2,)),
            pltpu.SemaphoreType.DMA((6,)),
            pltpu.SemaphoreType.DMA((blocks,)),
            pltpu.SemaphoreType.DMA((chunks, count)),
            pltpu.SemaphoreType.DMA((2, count // 2)),
            pltpu.SemaphoreType.DMA((chunks, count)),
            pltpu.SemaphoreType.DMA((n_high // 2,)),
            pltpu.SemaphoreType.DMA((n_high // 2,)),
        ],
        compiler_params=pltpu.CompilerParams(collective_id=0, has_side_effects=True),
    )(mix_angles, wave_parts, level_table, phase_angles)
    result, marginal = pl.pallas_call(
        finish,
        out_shape=[
            jax.ShapeDtypeStruct(wave_parts.shape, f32),
            jax.ShapeDtypeStruct((blocks, part, lanes), f32),
        ],
        in_specs=[vmem, vmem],
        out_specs=[any_space, any_space],
        scratch_shapes=[pltpu.SemaphoreType.DMA((2,))],
    )(*(pltpu.with_memory_space_constraint(x, pltpu.VMEM) for x in (back, total)))
    return (result, marginal)


def solution(mesh):
    in_specs = (P(None, ("high", "low"), None, None), P(("high", "low"), None, None), P(), P())
    out_specs = (P(None, ("high", "low"), None, None), P("low", "high", None))
    return jax.shard_map(
        functools.partial(on_device, mesh.shape["high"], mesh.shape["low"]),
        mesh=mesh, in_specs=in_specs, out_specs=out_specs, check_vma=False,
    )
```

```python
import functools

import jax
import jax.numpy as jnp
from jax import lax
from jax.experimental import pallas as pl
from jax.experimental.pallas import tpu as pltpu
from jax.sharding import PartitionSpec as P

LAYERS = 2
MESH = pl.DeviceIdType.MESH
SUBLANES = 8
TERMS = 5


def count_bits(values, count):
    places = jnp.arange(count.bit_length() - 1, dtype=jnp.int32)
    return jnp.sum(values[..., None] >> places & 1, axis=-1)


def real_turn_table(count, angle):
    rank = jnp.arange(count, dtype=jnp.int32)
    apart = count_bits(rank[:, None] ^ rank[None, :], count)
    minus = count_bits(rank[:, None] & (rank[:, None] ^ rank[None, :]), count)
    bits = count.bit_length() - 1
    size = jnp.cos(angle) ** (bits - apart).astype(jnp.float32) * jnp.sin(angle) ** apart.astype(
        jnp.float32
    )
    return size * jnp.where(minus % 2 == 1, -1.0, 1.0).astype(jnp.float32)


def apply_along(values, dim, angle):
    real_part = real_turn_table(values.shape[dim], angle)
    moved = jnp.tensordot(values, real_part, axes=([dim], [0]), precision=lax.Precision.HIGHEST)
    return jnp.moveaxis(moved, -1, dim)


def phase_step(values, levels, angle):
    turn = angle * levels
    return jnp.stack(
        [
            values[0] * jnp.cos(turn) + values[1] * jnp.sin(turn),
            values[1] * jnp.cos(turn) - values[0] * jnp.sin(turn),
        ]
    )


def by_axis(wave_parts, level_table, phase_angles, mix_angles):
    values = wave_parts
    for layer in range(LAYERS):
        values = phase_step(values, level_table, phase_angles[layer])
        values = apply_along(values, 3, mix_angles[layer, 0])
        values = apply_along(values, 2, mix_angles[layer, 1])
        values = apply_along(values, 1, mix_angles[layer, 2])
        moved = lax.all_to_all(values, "high", split_axis=2, concat_axis=1, tiled=True)
        spread = moved.reshape(2, lax.axis_size("high"), -1, moved.shape[2], moved.shape[3])
        moved = apply_along(spread, 1, mix_angles[layer, 2]).reshape(moved.shape)
        values = lax.all_to_all(moved, "high", split_axis=1, concat_axis=2, tiled=True)
        moved = lax.all_to_all(values, "low", split_axis=3, concat_axis=1, tiled=True)
        spread = moved.reshape(2, lax.axis_size("low"), -1, moved.shape[2], moved.shape[3])
        moved = apply_along(spread, 1, mix_angles[layer, 3]).reshape(moved.shape)
        values = lax.all_to_all(moved, "low", split_axis=1, concat_axis=3, tiled=True)
    chance = values[0] * values[0] + values[1] * values[1]
    marginal = lax.psum_scatter(chance, "high", scatter_dimension=1, tiled=True) / lax.axis_size(
        "high"
    )
    return (values, marginal)


def mix_list(values, groups):
    values = list(values)
    stride = 1
    for bits, cos, sin in groups:
        for _ in range(bits):
            for at in range(len(values)):
                if at & stride == 0:
                    u, v = values[at], values[at + stride]
                    values[at] = cos * u - sin * v
                    values[at + stride] = cos * v + sin * u
            stride *= 2
    return values


def series(square, first):
    terms = [1.0]
    for n in range(TERMS):
        terms.append(-terms[-1] / ((2 * n + first) * (2 * n + first + 1)))
    out = jnp.full_like(square, terms[-1])
    for term in terms[-2::-1]:
        out = out * square + term
    return out


def cos_sin(half):
    square = half * half
    cos, sin = series(square, 1), half * series(square, 2)
    twice = sin + sin
    return 1.0 - twice * sin, twice * cos


def turn_matrix(groups, sign):
    size = 1
    for bits, _, _ in groups:
        size <<= bits
    row = lax.broadcasted_iota(jnp.int32, (size, size), 0)
    column = lax.broadcasted_iota(jnp.int32, (size, size), 1)
    out = None
    place = 0
    for bits, cos, sin in groups:
        up = sign * sin
        for _ in range(bits):
            kb = (row >> place) & 1
            nb = (column >> place) & 1
            factor = jnp.where(kb == nb, cos, jnp.where(nb > kb, up, -up))
            out = factor if out is None else out * factor
            place += 1
    return out


def split(values):
    high = values.astype(jnp.bfloat16)
    return high, (values - high.astype(jnp.float32)).astype(jnp.bfloat16)


def dot(left, right):
    return jnp.dot(left, right, preferred_element_type=jnp.float32)


def xor(left, right):
    out = 0
    for bit in doublings(1, 64):
        out = out + (left // bit + right // bit) % 2 * bit
    return out


def doublings(first, end):
    return [1 << i for i in range(first.bit_length() - 1, end.bit_length() - 1)]


def log2(count):
    return count.bit_length() - 1


def turn_chunks(ref, t, h, part, pair):
    chunks = part // SUBLANES
    at = [pl.ds(h * part + j * SUBLANES, SUBLANES) for j in range(chunks)]
    return [mix_list([ref[p, t, r, :] for r in at], [(log2(chunks), *pair)]) for p in range(2)]


def finish(back, total, out_hbm, marginal_hbm, sem):
    copies = [
        pltpu.make_async_copy(back, out_hbm, sem.at[0]),
        pltpu.make_async_copy(total, marginal_hbm, sem.at[1]),
    ]
    for copy in copies:
        copy.start()
    for copy in copies:
        copy.wait()


def kernel(
    n_high, n_low,
    mix_hbm, wave_hbm, level_hbm, phase_hbm,
    back, total,
    mix_ref, phase_ref, wave_ref, level_ref, level_far, a_ref, b_ref, c_ref, level_b, chance, pair, sums, gathered,
    ready, load_sem, send_sem, recv_far, recv_state, recv_level, recv_back, recv_pair, recv_sums,
):
    loads = [
        pltpu.make_async_copy(level_hbm, level_ref, load_sem.at[0]),
        pltpu.make_async_copy(wave_hbm, wave_ref, load_sem.at[1]),
        pltpu.make_async_copy(phase_hbm, phase_ref, load_sem.at[2]),
        pltpu.make_async_copy(mix_hbm, mix_ref, load_sem.at[3]),
    ]
    for load in loads:
        load.start()
    _, blocks, rows, lanes = wave_ref.shape
    part = rows // n_high
    chunks = part // SUBLANES
    count = n_high * n_low
    twos = half = n_high // 2
    mh, ml = lax.axis_index("high"), lax.axis_index("low")

    barrier = pltpu.get_barrier_semaphore()

    def other(i):
        k = 1 + i
        return k, (mh + k // n_low) % n_high, (ml + k % n_low) % n_low

    mz, mc = mh // 2, mh % 2
    far = (mh + half) % n_high
    mine = mh // half * half

    steps = [(bit, 0) for bit in doublings(1, n_high)] + [(0, bit) for bit in doublings(1, n_low)]

    def across(step):
        return xor(mh, step[0]), xor(ml, step[1])

    for step in steps:
        pl.semaphore_signal(barrier, inc=1, device_id=across(step), device_id_type=MESH)

    def angles(layer, group):
        angle = jnp.full((SUBLANES, lanes), mix_ref[layer, group], jnp.float32)
        return jnp.cos(angle), jnp.sin(angle)

    def wide(pair, size):
        return tuple(jnp.broadcast_to(x[:1, :1], (size, size)) for x in pair)

    def phase(re, im, levels, layer):
        cos, sin = cos_sin(phase_ref[pl.ds(layer, 1), :] * 0.5 * levels)
        return re * cos + im * sin, im * cos - re * sin

    def tile(h, j):
        return pl.ds(pl.multiple_of(h * part + j * SUBLANES, SUBLANES), SUBLANES)

    def rows_of(h):
        return pl.ds(pl.multiple_of(h * part, SUBLANES), part)

    def mix_in_a(ref, j, layer):
        row_pair, block_pair = angles(layer, 1), angles(layer, 2)
        groups = [(log2(n_high), *row_pair), (log2(blocks), *block_pair)]
        at = [(t, tile(h, j)) for t in range(blocks) for h in range(n_high)]
        for p in range(2):
            values = mix_list([ref[p, t, r, :] for t, r in at], groups)
            for (t, r), value in zip(at, values):
                ref[p, t, r, :] = value

    def mix_chunks(ref, t, h, layer):
        return turn_chunks(ref, t, h, part, angles(layer, 1))

    def tables(layer):
        lane = split(turn_matrix([(log2(lanes), *wide(angles(layer, 0), lanes))], 1.0))
        packed = jnp.concatenate(
            [jnp.concatenate(lane, axis=1), jnp.concatenate([lane[0], jnp.zeros_like(lane[0])], axis=1)], axis=0
        )
        size = count * SUBLANES
        row_pair, block_pair, low_pair = (wide(angles(layer, g), size) for g in (1, 2, 3))
        upper = turn_matrix(
            [(log2(SUBLANES), *row_pair), (log2(n_high), *block_pair), (log2(n_low), *low_pair)], -1.0
        )
        return packed, split(upper)

    def mix_in_b(ref, j, packed, upper):
        size = count * SUBLANES
        both = jnp.concatenate([ref[j, p].reshape(size, lanes) for p in range(2)], axis=1)
        high, low = split(both)
        both = dot(upper[0], high) + (dot(upper[1], high) + dot(upper[0], low))
        rows = jnp.concatenate([both[:, :lanes], both[:, lanes:]], axis=0)
        out = dot(jnp.concatenate(split(rows), axis=1), packed)
        out = out[:, :lanes] + out[:, lanes:]
        for p in range(2):
            c_ref[j, p] = out[p * size : (p + 1) * size].reshape(n_low, n_high, SUBLANES, lanes)

    def state_copy(j, i):
        k, dh, dl = other(i)
        return pltpu.make_async_remote_copy(
            src_ref=a_ref.at[:, dl, tile(dh, j), :],
            dst_ref=b_ref.at[j, :, ml, mh],
            send_sem=send_sem.at[0],
            recv_sem=recv_state.at[j, k],
            device_id=(dh, dl),
            device_id_type=MESH,
        )

    def far_copy(t):
        return pltpu.make_async_remote_copy(
            src_ref=level_ref.at[t, pl.ds(pl.multiple_of((half - mine) * part, SUBLANES), half * part), :],
            dst_ref=level_far.at[t],
            send_sem=send_sem.at[5],
            recv_sem=recv_far.at[t],
            device_id=(far, ml),
            device_id_type=MESH,
        )

    def level_copy(whose, i):
        k = 1 + i
        dh, dl = (mh - mine + k // n_low) % half, (ml + k % n_low) % n_low
        return pltpu.make_async_remote_copy(
            src_ref=[level_ref.at[dl, rows_of(mine + dh), :], level_far.at[dl, rows_of(dh), :]][whose],
            dst_ref=level_b.at[ml, [mh, far][whose]],
            send_sem=send_sem.at[1],
            recv_sem=recv_level.at[whose, k],
            device_id=(mine + dh, dl),
            device_id_type=MESH,
        )

    def back_copy(j, i):
        k, dh, dl = other(i)
        return pltpu.make_async_remote_copy(
            src_ref=c_ref.at[j, :, dl, dh],
            dst_ref=back.at[:, ml, tile(mh, j), :],
            send_sem=send_sem.at[2],
            recv_sem=recv_back.at[j, k],
            device_id=(dh, dl),
            device_id_type=MESH,
        )

    def each(do, copy, j):
        for i in range(half * n_low - 1 if copy is level_copy else count - 1):
            getattr(copy(j, i), do)()

    rounds = [step for step in steps if step != (half, 0)]

    def tell(i):
        pl.semaphore_signal(ready.at[i], inc=1, device_id=across(rounds[i]), device_id_type=MESH)

    def hear(i):
        pl.semaphore_wait(ready.at[i], 1)

    loads[0].wait()
    pl.semaphore_wait(barrier, len(steps))
    for t in range(blocks):
        far_copy(t).start()
    tell(0)
    for load in loads[1:]:
        load.wait()
    for i in range(1, len(rounds) - 1):
        hear(i - 1)
        tell(i)

    @pl.loop(0, blocks * rows // 32)
    def _(i):
        t, r = i // (rows // 32), pl.ds(pl.multiple_of(i % (rows // 32) * 32, 32), 32)
        re, im = phase(wave_ref[0, t, r, :], wave_ref[1, t, r, :], level_ref[t, r, :], 0)
        a_ref[0, t, r, :] = re
        a_ref[1, t, r, :] = im

    hear(len(rounds) - 2)
    tell(len(rounds) - 1)

    @pl.loop(0, chunks)
    def _(j):
        mix_in_a(a_ref, j, 0)

    @pl.loop(0, blocks)
    def _(t):
        for h in range(n_high):
            for p, values in enumerate(mix_chunks(a_ref, t, h, 0)):
                for j, value in enumerate(values):
                    a_ref[p, t, tile(h, j), :] = value

    hear(len(rounds) - 1)
    each("start", state_copy, 0)
    each("start", level_copy, 0)
    first, second = tables(0), tables(1)
    for j in range(chunks):
        b_ref[j, :, ml, mh] = a_ref[:, ml, tile(mh, j), :]
    level_b[ml, mh] = level_ref[ml, rows_of(mh), :]
    for t in range(blocks):
        far_copy(t).wait_recv()
    each("start", level_copy, 1)
    for j in range(1, chunks):
        each("start", state_copy, j)
    level_b[ml, far] = level_far[ml, rows_of(mh - mine), :]

    for j in range(chunks):
        each("wait_recv", state_copy, j)
        mix_in_b(b_ref, j, *first)
        if j == 0:
            each("wait_recv", level_copy, 0)
            each("wait_recv", level_copy, 1)

        @pl.loop(0, n_low)
        def _(l):
            levels = level_b[l, :, j * SUBLANES : (j + 1) * SUBLANES, :]
            re, im = phase(c_ref[j, 0, l], c_ref[j, 1, l], levels, 1)
            c_ref[j, 0, l] = re
            c_ref[j, 1, l] = im

        mix_in_b(c_ref, j, *second)
        each("start", back_copy, j)
        back[:, ml, tile(mh, j), :] = c_ref[j, :, ml, mh]

    for j in range(chunks):
        each("wait_send", state_copy, j)
    for whose in range(2):
        each("wait_send", level_copy, whose)
    for t in range(blocks):
        far_copy(t).wait_send()

    for j in range(chunks):
        each("wait_recv", back_copy, j)
        mix_in_a(back, j, 1)

    @pl.loop(0, blocks)
    def _(t):
        for h in range(n_high):
            re, im = mix_chunks(back, t, h, 1)
            for j in range(chunks):
                back[0, t, tile(h, j), :] = re[j]
                back[1, t, tile(h, j), :] = im[j]
                chance[h % 2, h // 2, t, pl.ds(j * SUBLANES, SUBLANES), :] = re[j] * re[j] + im[j] * im[j]

    def pair_copy(i):
        dz = (mz + i + 1) % twos
        return dz, pltpu.make_async_remote_copy(
            src_ref=chance.at[mc, dz],
            dst_ref=pair.at[dz],
            send_sem=send_sem.at[3],
            recv_sem=recv_pair.at[i],
            device_id=(mz * 2 + 1 - mc, ml),
            device_id_type=MESH,
        )

    def sums_copy(i):
        dz = (mz + i + 1) % twos
        return pltpu.make_async_remote_copy(
            src_ref=sums.at[dz],
            dst_ref=gathered.at[mz],
            send_sem=send_sem.at[4],
            recv_sem=recv_sums.at[i],
            device_id=(dz * 2 + 1 - mc, ml),
            device_id_type=MESH,
        )

    for i in range(twos):
        pair_copy(i)[1].start()
    for i in range(twos):
        dz, copy = pair_copy(i)
        copy.wait_recv()
        sums[dz] = chance[1 - mc, dz] + pair[dz]
        sums_copy(i).start()
    for j in range(chunks):
        each("wait_send", back_copy, j)
    for i in range(twos):
        pair_copy(i)[1].wait_send()
    for i in range(twos):
        sums_copy(i).wait_recv()
    summed = gathered[0]
    for z in range(1, twos):
        summed = summed + gathered[z]
    total[...] = summed * (1.0 / n_high)
    for i in range(twos):
        sums_copy(i).wait_send()


def on_device(n_high, n_low, wave_parts, level_table, phase_angles, mix_angles):
    _, blocks, rows, lanes = wave_parts.shape
    if blocks != n_low or n_high < 4 or n_high & (n_high - 1) or rows % (n_high * SUBLANES):
        return by_axis(wave_parts, level_table, phase_angles, mix_angles)
    part = rows // n_high
    chunks = part // SUBLANES
    count = n_high * n_low
    f32 = jnp.float32
    vmem = pl.BlockSpec(memory_space=pltpu.VMEM)
    any_space = pl.BlockSpec(memory_space=pl.ANY)
    back, total = pl.pallas_call(
        functools.partial(kernel, n_high, n_low),
        out_shape=[
            pltpu.VMEM(wave_parts.shape, f32),
            pltpu.VMEM((blocks, part, lanes), f32),
        ],
        in_specs=[any_space] * 4,
        out_specs=[vmem, vmem],
        scratch_shapes=[
            pltpu.SMEM(mix_angles.shape, f32),
            pltpu.VMEM(phase_angles.shape, f32),
            pltpu.VMEM((2, blocks, rows, lanes), f32),
            pltpu.VMEM((blocks, rows, lanes), f32),
            pltpu.VMEM((blocks, rows // 2, lanes), f32),
            pltpu.VMEM((2, blocks, rows, lanes), f32),
            pltpu.VMEM((chunks, 2, n_low, n_high, SUBLANES, lanes), f32),
            pltpu.VMEM((chunks, 2, n_low, n_high, SUBLANES, lanes), f32),
            pltpu.VMEM((n_low, n_high, part, lanes), f32),
            pltpu.VMEM((2, n_high // 2, blocks, part, lanes), f32),
            pltpu.VMEM((n_high // 2, blocks, part, lanes), f32),
            pltpu.VMEM((n_high // 2, blocks, part, lanes), f32),
            pltpu.VMEM((n_high // 2, blocks, part, lanes), f32),
            pltpu.SemaphoreType.REGULAR((log2(count) - 1,)),
            pltpu.SemaphoreType.DMA((4,)),
            pltpu.SemaphoreType.DMA((6,)),
            pltpu.SemaphoreType.DMA((blocks,)),
            pltpu.SemaphoreType.DMA((chunks, count)),
            pltpu.SemaphoreType.DMA((2, count // 2)),
            pltpu.SemaphoreType.DMA((chunks, count)),
            pltpu.SemaphoreType.DMA((n_high // 2,)),
            pltpu.SemaphoreType.DMA((n_high // 2,)),
        ],
        compiler_params=pltpu.CompilerParams(collective_id=0, has_side_effects=True),
    )(mix_angles, wave_parts, level_table, phase_angles)
    result, marginal = pl.pallas_call(
        finish,
        out_shape=[
            jax.ShapeDtypeStruct(wave_parts.shape, f32),
            jax.ShapeDtypeStruct((blocks, part, lanes), f32),
        ],
        in_specs=[vmem, vmem],
        out_specs=[any_space, any_space],
        scratch_shapes=[pltpu.SemaphoreType.DMA((2,))],
    )(*(pltpu.with_memory_space_constraint(x, pltpu.VMEM) for x in (back, total)))
    return (result, marginal)


def solution(mesh):
    in_specs = (P(None, ("high", "low"), None, None), P(("high", "low"), None, None), P(), P())
    out_specs = (P(None, ("high", "low"), None, None), P("low", "high", None))
    return jax.shard_map(
        functools.partial(on_device, mesh.shape["high"], mesh.shape["low"]),
        mesh=mesh, in_specs=in_specs, out_specs=out_specs, check_vma=False,
    )
```
